8 devices in a mesh: dp: 2 (over y, z), tp: 4 (over x, core).
Axes of the slice: x: 2, y: 2, z: 1, core: 2. Of those that a mesh axis runs over, the one named last changes fastest.
Arguments:
- x: bfloat16 [4096, 2048], P('dp'), parts along dimension 0
- gain: bfloat16 [2048], replicated
- wq: bfloat16 [2048, 3072], P(None, 'tp')
- wk: bfloat16 [2048, 3072], P(None, 'tp')
- wv: bfloat16 [2048, 3072], P(None, 'tp')
- wo: bfloat16 [3072, 2048], P('tp')
Outputs:
- output: bfloat16 [4096, 2048], P('dp'), parts along dimension 0
There are 2 independent parts. The reference program is written for one: setup_inputs(seed, part) draws one part's arguments, and reference() takes and returns one part's arrays. A program takes and returns all parts, laid end to end along the dimension named above; an argument that names none is the same for every part.
All inputs are finite; a program needn't handle non-finite values.
Results may differ from the reference program's by a relative error of at most 0.012.
Values are sent between devices in bfloat16 or wider.
A program may use at most 2 GiB of HBM per device.

```python
import jax
import jax.numpy as jnp
from jax import lax

ROWS = 2048
D = 2048
HEADS = 24
KV_HEADS = 24
HEAD = 128
THETA = 10000


def setup_inputs(seed: int = 0, part: int = 0) -> dict:
    kx, kn, kq, kk, kv, ko = jax.random.split(jax.random.key(seed), 6)

    def weights(key, rows, columns):
        return jax.random.normal(key, (rows, columns), jnp.float32) * rows**-0.5

    drawn = {
        "x": jax.random.normal(jax.random.fold_in(kx, part), (ROWS, D), jnp.float32),
        "gain": 1 + 0.1 * jax.random.normal(kn, (D,), jnp.float32),
        "wq": 2 * weights(kq, D, HEADS * HEAD),
        "wk": 2 * weights(kk, D, KV_HEADS * HEAD),
        "wv": 4 * weights(kv, D, KV_HEADS * HEAD),
        "wo": weights(ko, HEADS * HEAD, D),
    }
    return {k: v.astype(jnp.bfloat16) for k, v in drawn.items()}


def normed(x, gain):
    wide = x.astype(jnp.float32)
    scale = lax.rsqrt(jnp.mean(wide * wide, -1, keepdims=True) + 1e-6)
    return (wide * scale * gain.astype(jnp.float32)).astype(jnp.bfloat16)


def turned(t, place, theta):
    half = t.shape[-1] // 2
    angle = place.astype(jnp.float32)[:, None] * theta ** (-jnp.arange(half, dtype=jnp.float32) / half)
    cos, sin = jnp.cos(angle)[:, None], jnp.sin(angle)[:, None]
    a, b = t[..., :half].astype(jnp.float32), t[..., half:].astype(jnp.float32)
    return jnp.concatenate([a * cos - b * sin, b * cos + a * sin], -1).astype(jnp.bfloat16)


def matmul(a, w):
    return jnp.dot(a, w, preferred_element_type=jnp.float32).astype(jnp.bfloat16)


def einsum(form, a, b):
    return jnp.einsum(form, a.astype(jnp.float32), b.astype(jnp.float32))


def attention(q, k, v):
    scores = einsum("tgsd,ugd->gstu", q, k) * q.shape[-1] ** -0.5
    token = jnp.arange(q.shape[0])
    scores = jnp.where(token[:, None] >= token, scores, -jnp.inf)
    weights = jax.nn.softmax(scores, -1).astype(jnp.bfloat16)
    return einsum("gstu,ugd->tgsd", weights, v).astype(jnp.bfloat16)


def reference(x, gain, wq, wk, wv, wo):
    a, place = normed(x, gain), jnp.arange(ROWS)
    q = turned(matmul(a, wq).reshape(ROWS, HEADS, HEAD), place, THETA).reshape(ROWS, KV_HEADS, -1, HEAD)
    k = turned(matmul(a, wk).reshape(ROWS, KV_HEADS, HEAD), place, THETA)
    v = matmul(a, wv).reshape(ROWS, KV_HEADS, HEAD)
    seen = attention(q, k, v).reshape(ROWS, HEADS * HEAD)
    return (x.astype(jnp.float32) + jnp.dot(seen, wo, preferred_element_type=jnp.float32)).astype(jnp.bfloat16)
```

```python
import functools

import jax
import jax.numpy as jnp
import numpy as np
from jax import lax
from jax.experimental import pallas as pl
from jax.experimental.pallas import tpu as pltpu
from jax.sharding import PartitionSpec as P

HEAD = 128
THETA = 10000
LOG2E = 1.4426950408889634
BLK = 256
HALF = BLK // 2
ONES = 16
MESH = pl.DeviceIdType.MESH
BF, F32 = jnp.bfloat16, jnp.float32


def _dot(a, b, ca, cb):
    return lax.dot_general(a, b, (((ca,), (cb,)), ((), ())), preferred_element_type=F32)


def tables(rows):
    half = HEAD // 2
    angle = np.arange(rows)[:, None] * THETA ** (-np.arange(half) / half)
    cos, sin = np.cos(angle), np.sin(angle)
    return np.concatenate([cos, cos], 1).astype(np.float32), np.concatenate([-sin, sin], 1).astype(np.float32)


def kernel(nb, heads, x_h, gain_ref, cos_h, sin_h, wq_h, wk_h, wv_h, wo_h, y_h,
           x_s, cos_s, sin_s, wq_s, wk_s, wv_s, wo_s, xn_s, q_s, k_s, v_s, top_s, mix_s, seen_s, part_s, own_s,
           psend, precv, csend, crecv,
           x_sem, t_sem, w_sem, ps_sem, pr_sem, cs_sem, cr_sem, fs_sem, fr_sem, y_sem):
    me = lax.axis_index("tp")
    core = lax.rem(me, 2)
    partner = me + 1 - 2 * core
    across = lax.rem(me + 2, 4)
    d = x_s.shape[1]
    width = heads * HEAD
    e = HEAD**-0.5 * LOG2E

    def rows(i):
        return pl.ds(pl.multiple_of(i * BLK, BLK), BLK)

    def mine(i):
        return pl.ds(pl.multiple_of(i * BLK + core * HALF, HALF), HALF)

    def load_x(i):
        return pltpu.make_async_copy(x_h.at[rows(i)], x_s.at[rows(i)], x_sem.at[i])

    weights = [pltpu.make_async_copy(a, b, w_sem.at[n]) for n, (a, b) in
               enumerate([(wq_h, wq_s), (wk_h, wk_s), (wv_h, wv_s), (wo_h, wo_s)])]
    turns = [pltpu.make_async_copy(a, b, t_sem.at[n]) for n, (a, b) in enumerate([(cos_h, cos_s), (sin_h, sin_s)])]
    load_x(0).start()
    weights[0].start()
    for c in turns:
        c.start()
    for c in weights[1:]:
        c.start()

    barrier = pltpu.get_barrier_semaphore()
    for other in (partner, across):
        pl.semaphore_signal(barrier, inc=1, device_id={"tp": other}, device_id_type=MESH)
    pl.semaphore_wait(barrier, 2)

    def to_partner(i):
        return pltpu.make_async_remote_copy(psend.at[i], precv.at[i], ps_sem.at[i], pr_sem.at[i], device_id={"tp": partner}, device_id_type=MESH)

    def to_across(i):
        return pltpu.make_async_remote_copy(csend.at[i], crecv.at[i], cs_sem.at[i], cr_sem.at[i], device_id={"tp": across}, device_id_type=MESH)

    def chip_sum(i):
        to_partner(i).wait_recv()

        def strip(r, _):
            at = pl.ds(pl.multiple_of(r * 32, 32), 32)
            csend[i, at, :] = (own_s[lax.rem(i, 2), at, :] + precv[i, at, :].astype(F32)).astype(BF)

        lax.fori_loop(0, HALF // 32, strip, None)
        to_across(i).start()

    def turned(t, cos, sin):
        t = t.astype(BF).astype(F32)
        return (t * cos + pltpu.roll(t, HEAD // 2, 1) * sin).astype(BF)

    def attend(i, j, masked, first):
        scores = [_dot(k_s[j, h], q_s[h], 1, 1) for h in range(heads)]
        if masked:
            ok = lax.broadcasted_iota(jnp.int32, (BLK, BLK), 0) <= lax.broadcasted_iota(jnp.int32, (BLK, BLK), 1)
        ps, keeps = [], []
        for h, s in enumerate(scores):
            if masked:
                s = jnp.where(ok, s, -1e30)
            top = s.max(axis=0, keepdims=True)
            if not first:
                old = top_s[h : h + 1, :]
                top = jnp.maximum(old, top)
                keeps.append(jnp.exp2((old - top) * e))
            top_s[h : h + 1, :] = top
            ps.append(jnp.exp2((s - top) * e).astype(BF))
        for h in range(heads):
            new = _dot(v_s[j, h], ps[h], 1, 0)
            mix_s[h] = new if first else mix_s[h] * keeps[h] + new

    def block(i, _):
        load_x(i).wait()

        @pl.when(i + 1 < nb)
        def _():
            load_x(jnp.minimum(i + 1, nb - 1)).start()

        def norm(r, _):
            wide = x_s[pl.ds(pl.multiple_of(i * BLK + r * 32, 32), 32), :].astype(F32)
            scale = lax.rsqrt(jnp.mean(wide * wide, -1, keepdims=True) + 1e-6)
            xn_s[pl.ds(pl.multiple_of(r * 32, 32), 32), :] = (wide * scale * gain_ref[...].astype(F32)).astype(BF)

        lax.fori_loop(0, BLK // 32, norm, None)

        @pl.when(i == 0)
        def _():
            weights[0].wait()
            for c in turns:
                c.wait()

        cos, sin = cos_s[rows(i), :], sin_s[rows(i), :]
        xn = xn_s[...]
        for at in range(0, width, 256):
            t = _dot(xn, wq_s[:, at : at + 256], 1, 0)
            for n in range(2):
                q_s[at // HEAD + n] = turned(t[:, n * HEAD : (n + 1) * HEAD], cos, sin)

        @pl.when(i == 0)
        def _():
            weights[1].wait()

        for at in range(0, width, 256):
            t = _dot(xn, wk_s[:, at : at + 256], 1, 0)
            for n in range(2):
                k_s[i, at // HEAD + n] = turned(t[:, n * HEAD : (n + 1) * HEAD], cos, sin)

        @pl.when(i == 0)
        def _():
            weights[2].wait()

        for at in range(0, width, 256):
            t = _dot(xn, wv_s[:, at : at + 256], 1, 0).astype(BF).T
            for n in range(2):
                v_s[i, at // HEAD + n, :HEAD, :] = t[n * HEAD : (n + 1) * HEAD, :]
                v_s[i, at // HEAD + n, HEAD:, :] = jnp.ones((ONES, BLK), BF)

        @pl.when(i > 1)
        def _():
            chip_sum(jnp.maximum(i - 1, 0))

        attend(i, i, True, True)
        lax.fori_loop(0, i, lambda j, _: attend(i, j, False, False), None)
        for h in range(heads):
            out = mix_s[h, :HEAD, :] * (1 / mix_s[h, HEAD : HEAD + 1, :])
            seen_s[:, h * HEAD : (h + 1) * HEAD] = out.astype(BF).T

        @pl.when(i == 0)
        def _():
            weights[3].wait()

        seen = seen_s[...]
        for at in range(0, d, 512):
            part_s[:, at : at + 512] = _dot(seen, wo_s[:, at : at + 512], 1, 0)

        def split(r, _):
            at = pl.ds(pl.multiple_of(r * 32, 32), 32)
            own_s[lax.rem(i, 2), at, :] = part_s[pl.ds(pl.multiple_of(core * HALF + r * 32, 32), 32), :]
            psend[i, at, :] = part_s[pl.ds(pl.multiple_of((1 - core) * HALF + r * 32, 32), 32), :].astype(BF)

        lax.fori_loop(0, HALF // 32, split, None)
        to_partner(i).start()

        @pl.when(i == 0)
        def _():
            chip_sum(0)


    lax.fori_loop(0, nb, block, None)
    chip_sum(nb - 1)

    def finals(i):
        return (pltpu.make_async_copy(psend.at[i], y_h.at[mine(i)], y_sem.at[i]),
                pltpu.make_async_remote_copy(psend.at[i], y_h.at[mine(i)], fs_sem.at[i], fr_sem.at[i], device_id={"tp": partner}, device_id_type=MESH))

    def finish(i, _):
        to_partner(i).wait_send()
        to_across(i).wait()

        def strip(r, _):
            at = pl.ds(pl.multiple_of(r * 32, 32), 32)
            total = csend[i, at, :].astype(F32) + crecv[i, at, :].astype(F32)
            here = pl.ds(pl.multiple_of(i * BLK + core * HALF + r * 32, 32), 32)
            psend[i, at, :] = (x_s[here, :].astype(F32) + total).astype(BF)

        lax.fori_loop(0, HALF // 32, strip, None)
        for c in finals(i):
            c.start()

    lax.fori_loop(0, nb, finish, None)

    def drain(i, _):
        for c in finals(i):
            c.wait()

    lax.fori_loop(0, nb, drain, None)


def solution(mesh):
    def step(x, gain, wq, wk, wv, wo):
        rows, d = x.shape
        width = wq.shape[1]
        heads, nb = width // HEAD, rows // BLK
        cos, sin = (jnp.asarray(t) for t in tables(rows))
        anywhere, dma = pl.BlockSpec(memory_space=pl.ANY), pltpu.SemaphoreType.DMA
        return pl.pallas_call(
            functools.partial(kernel, nb, heads),
            name="layer",
            out_shape=jax.ShapeDtypeStruct((rows, d), BF),
            in_specs=[anywhere, pl.BlockSpec(memory_space=pltpu.VMEM)] + [anywhere] * 6,
            out_specs=anywhere,
            scratch_shapes=[
                pltpu.VMEM((rows, d), BF), pltpu.VMEM((rows, HEAD), F32), pltpu.VMEM((rows, HEAD), F32),
                pltpu.VMEM((d, width), BF), pltpu.VMEM((d, width), BF), pltpu.VMEM((d, width), BF), pltpu.VMEM((width, d), BF),
                pltpu.VMEM((BLK, d), BF), pltpu.VMEM((heads, BLK, HEAD), BF), pltpu.VMEM((nb, heads, BLK, HEAD), BF),
                pltpu.VMEM((nb, heads, HEAD + ONES, BLK), BF), pltpu.VMEM((8, BLK), F32),
                pltpu.VMEM((heads, HEAD + ONES, BLK), F32), pltpu.VMEM((BLK, width), BF),
                pltpu.VMEM((BLK, d), F32), pltpu.VMEM((2, HALF, d), F32),
                *[pltpu.VMEM((nb, HALF, d), BF)] * 4,
                dma((nb,)), dma((2,)), dma((4,)), *[dma((nb,))] * 7,
            ],
            compiler_params=pltpu.CompilerParams(collective_id=0, has_side_effects=True, vmem_limit_bytes=63 * 2**20),
        )(x, gain.reshape(1, d), cos, sin, wq, wk, wv, wo)

    tokens, columns = P("dp", None), P(None, "tp")
    return jax.shard_map(
        step,
        mesh=mesh,
        in_specs=(tokens, P(None), columns, columns, columns, P("tp", None)),
        out_specs=tokens,
        check_vma=False,
    )
```

```python
import functools

import jax
import jax.numpy as jnp
import numpy as np
from jax import lax
from jax.experimental import pallas as pl
from jax.experimental.pallas import tpu as pltpu
from jax.sharding import PartitionSpec as P

HEAD = 128
THETA = 10000
LOG2E = 1.4426950408889634
BLK = 256
HALF = BLK // 2
COLS = 512
ONES = 16
MESH = pl.DeviceIdType.MESH
BF, F32 = jnp.bfloat16, jnp.float32


def _dot(a, b, ca, cb):
    return lax.dot_general(a, b, (((ca,), (cb,)), ((), ())), preferred_element_type=F32)


def tables(rows):
    half = HEAD // 2
    angle = np.arange(rows)[:, None] * THETA ** (-np.arange(half) / half)
    cos, sin = np.cos(angle), np.sin(angle)
    return np.concatenate([cos, cos], 1).astype(np.float32), np.concatenate([-sin, sin], 1).astype(np.float32)


def kernel(nb, heads, x_h, gain_ref, cos_h, sin_h, wq_h, wk_h, wv_h, wo_h, y_ref,
           x_s, cos_s, sin_s, wq_s, wk_s, wv_s, wo_s, xn_s, q_s, k_s, v_s, s_s, top_s, mix_s, seen_s, own_s,
           precv, csend, crecv,
           x_sem, t_sem, w_sem, ps_sem, pr_sem, cs_sem, cr_sem, fs_sem, fr_sem, r_sem):
    me = lax.axis_index("tp")
    core = lax.rem(me, 2)
    partner = me + 1 - 2 * core
    across = lax.rem(me + 2, 4)
    d = x_s.shape[2]
    nc = d // COLS
    width = heads * HEAD
    e = HEAD**-0.5 * LOG2E

    def rows(i):
        return pl.ds(pl.multiple_of(i * BLK, BLK), BLK)

    def mine(i):
        return pl.ds(pl.multiple_of(i * BLK + core * HALF, HALF), HALF)

    def cols(c):
        return pl.ds(c * COLS, COLS)

    def load_x(i):
        at = lax.rem(i, 2)
        return pltpu.make_async_copy(x_h.at[rows(jnp.minimum(i, nb - 1))], x_s.at[at], x_sem.at[at])

    weights = [pltpu.make_async_copy(a, b, w_sem.at[n]) for n, (a, b) in
               enumerate([(wq_h, wq_s), (wk_h, wk_s), (wv_h, wv_s), (wo_h, wo_s)])]
    turns = [pltpu.make_async_copy(a, b, t_sem.at[n]) for n, (a, b) in enumerate([(cos_h, cos_s), (sin_h, sin_s)])]
    load_x(0).start()
    weights[0].start()
    for c in turns:
        c.start()
    for c in weights[1:]:
        c.start()

    barrier = pltpu.get_barrier_semaphore()
    for other in (partner, across):
        pl.semaphore_signal(barrier, inc=1, device_id={"tp": other}, device_id_type=MESH)

    v_s[:, :, HEAD:, :] = jnp.ones((nb, heads, ONES, BLK), BF)
    pl.semaphore_wait(barrier, 2)

    def to_partner(i, c):
        return pltpu.make_async_remote_copy(y_ref.at[mine(i), cols(c)], precv.at[i, c], ps_sem.at[i, c], pr_sem.at[i, c],
                                            device_id={"tp": partner}, device_id_type=MESH)

    def to_across(i, c):
        return pltpu.make_async_remote_copy(csend.at[i, c], crecv.at[i, c], cs_sem.at[i, c], cr_sem.at[i, c],
                                            device_id={"tp": across}, device_id_type=MESH)

    def final(i, c):
        return pltpu.make_async_remote_copy(y_ref.at[mine(i), cols(c)], y_ref.at[mine(i), cols(c)], fs_sem.at[i, c], fr_sem.at[i, c],
                                            device_id={"tp": partner}, device_id_type=MESH)

    def residual(i, c):
        return pltpu.make_async_copy(x_h.at[mine(i), cols(c)], precv.at[i, c], r_sem.at[i, c])

    def chip_sum(i):
        for c in range(nc):
            to_partner(i, c).wait_recv()
            csend[i, c] = (own_s[lax.rem(i, 2), c] + precv[i, c].astype(F32)).astype(BF)
            to_across(i, c).start()
            residual(i, c).start()

    def norm(i):
        at = lax.rem(i, 2)
        for r in range(0, BLK, 32):
            wide = x_s[at, r : r + 32, :].astype(F32)
            scale = lax.rsqrt(jnp.mean(wide * wide, -1, keepdims=True) + 1e-6)
            xn_s[at, r : r + 32, :] = (wide * scale * gain_ref[...].astype(F32)).astype(BF)

    def turned(t, cos, sin):
        t = t.astype(BF).astype(F32)
        return (t * cos + pltpu.roll(t, HEAD // 2, 1) * sin).astype(BF)

    def scores(j, h):
        return _dot(k_s[j, h], q_s[h], 1, 1)

    def diagonal(i, more):
        ok = lax.broadcasted_iota(jnp.int32, (BLK, BLK), 0) <= lax.broadcasted_iota(jnp.int32, (BLK, BLK), 1)
        found = [scores(i, h) for h in range(heads)]
        if more:
            for h in range(heads):
                s_s[0, h] = scores(0, h)
        ps = []
        for h, s in enumerate(found):
            s = jnp.where(ok, s, -1e30)
            top = s.max(axis=0, keepdims=True)
            top_s[h : h + 1, :] = top
            ps.append(jnp.exp2((s - top) * e).astype(BF))
        for h in range(heads):
            mix_s[h] = _dot(v_s[i, h], ps[h], 1, 0)

    def attend(j, _):
        now, later = lax.rem(j, 2), lax.rem(j + 1, 2)
        ps, keeps = [], []
        for h in range(heads):
            s_s[later, h] = scores(j + 1, h)
            s = s_s[now, h]
            old = top_s[h : h + 1, :]
            top = jnp.maximum(old, s.max(axis=0, keepdims=True))
            top_s[h : h + 1, :] = top
            keeps.append(jnp.exp2((old - top) * e))
            ps.append(jnp.exp2((s - top) * e).astype(BF))
        for h in range(heads):
            mix_s[h] = mix_s[h] * keeps[h] + _dot(v_s[j, h], ps[h], 1, 0)

    def block(i, start):
        load_x(i + 1).start()
        now = lax.rem(i, 2)
        if start:
            weights[0].wait()
            for c in turns:
                c.wait()
        cos, sin = cos_s[rows(i), :], sin_s[rows(i), :]
        xn = xn_s[now]
        for at in range(0, width, 256):
            t = _dot(xn, wq_s[:, at : at + 256], 1, 0)
            for n in range(2):
                q_s[at // HEAD + n] = turned(t[:, n * HEAD : (n + 1) * HEAD], cos, sin)
        if start:
            weights[1].wait()
        for at in range(0, width, 256):
            t = _dot(xn, wk_s[:, at : at + 256], 1, 0)
            for n in range(2):
                k_s[i, at // HEAD + n] = turned(t[:, n * HEAD : (n + 1) * HEAD], cos, sin)
        if start:
            weights[2].wait()
        for at in range(0, width, 256):
            t = _dot(xn, wv_s[:, at : at + 256], 1, 0).astype(BF).T
            for n in range(2):
                v_s[i, at // HEAD + n, :HEAD, :] = t[n * HEAD : (n + 1) * HEAD, :]

        diagonal(i, not start)
        if not start:
            @pl.when(i > 1)
            def _():
                chip_sum(i - 1)

            lax.fori_loop(0, i, attend, None)
        for h in range(heads):
            out = mix_s[h, :HEAD, :] * (1 / mix_s[h, HEAD : HEAD + 1, :])
            out = out.astype(BF).T
            for n in range(2):
                to = core if n == 0 else 1 - core
                seen_s[pl.ds(pl.multiple_of(to * HALF, HALF), HALF), h * HEAD : (h + 1) * HEAD] = out[n * HALF : (n + 1) * HALF]

        if start:
            weights[3].wait()
        load_x(i + 1).wait()
        seen = seen_s[...]
        for c in range(nc):
            part = _dot(seen, wo_s[:, c * COLS : (c + 1) * COLS], 1, 0)
            own_s[now, c] = part[:HALF]
            y_ref[mine(i), c * COLS : (c + 1) * COLS] = part[HALF:].astype(BF)
            if start:
                to_partner(i, c).start()
        norm(i + 1)
        if start:
            chip_sum(i)
        else:
            for c in range(nc):
                to_partner(i, c).start()

    load_x(0).wait()
    norm(0)
    block(0, True)

    def later(i, _):
        block(i, False)

    lax.fori_loop(1, nb, later, None)
    chip_sum(nb - 1)

    def finish(i, _):
        for c in range(nc):
            to_partner(i, c).wait_send()
            residual(i, c).wait()
            to_across(i, c).wait()
            y_ref[mine(i), c * COLS : (c + 1) * COLS] = (
                precv[i, c].astype(F32) + (csend[i, c].astype(F32) + crecv[i, c].astype(F32))).astype(BF)
            final(i, c).start()

    lax.fori_loop(0, nb, finish, None)

    def drain(i, _):
        for c in range(nc):
            final(i, c).wait()

    lax.fori_loop(0, nb, drain, None)


def solution(mesh):
    def step(x, gain, wq, wk, wv, wo):
        rows, d = x.shape
        width = wq.shape[1]
        heads, nb, nc = width // HEAD, rows // BLK, d // COLS
        cos, sin = (jnp.asarray(t) for t in tables(rows))
        anywhere, vmem, dma = pl.BlockSpec(memory_space=pl.ANY), pl.BlockSpec(memory_space=pltpu.VMEM), pltpu.SemaphoreType.DMA
        return pl.pallas_call(
            functools.partial(kernel, nb, heads),
            name="layer",
            out_shape=pltpu.VMEM((rows, d), BF),
            in_specs=[anywhere, vmem] + [anywhere] * 6,
            out_specs=vmem,
            scratch_shapes=[
                pltpu.VMEM((2, BLK, d), BF), pltpu.VMEM((rows, HEAD), F32), pltpu.VMEM((rows, HEAD), F32),
                pltpu.VMEM((d, width), BF), pltpu.VMEM((d, width), BF), pltpu.VMEM((d, width), BF), pltpu.VMEM((width, d), BF),
                pltpu.VMEM((2, BLK, d), BF), pltpu.VMEM((heads, BLK, HEAD), BF), pltpu.VMEM((nb, heads, BLK, HEAD), BF),
                pltpu.VMEM((nb, heads, HEAD + ONES, BLK), BF), pltpu.VMEM((2, heads, BLK, BLK), F32), pltpu.VMEM((8, BLK), F32),
                pltpu.VMEM((heads, HEAD + ONES, BLK), F32), pltpu.VMEM((BLK, width), BF),
                pltpu.VMEM((2, nc, HALF, COLS), F32),
                *[pltpu.VMEM((nb, nc, HALF, COLS), BF)] * 3,
                dma((2,)), dma((2,)), dma((4,)), *[dma((nb, nc))] * 7,
            ],
            compiler_params=pltpu.CompilerParams(collective_id=0, has_side_effects=True, vmem_limit_bytes=55 * 2**20),
        )(x, gain.reshape(1, d), cos, sin, wq, wk, wv, wo)

    tokens, columns = P("dp", None), P(None, "tp")
    return jax.shard_map(
        step,
        mesh=mesh,
        in_specs=(tokens, P(None), columns, columns, columns, P("tp", None)),
        out_specs=tokens,
        check_vma=False,
    )
```

```python
import functools

import jax
import jax.numpy as jnp
import numpy as np
from jax import lax
from jax.experimental import pallas as pl
from jax.experimental.pallas import tpu as pltpu
from jax.sharding import PartitionSpec as P

HEAD = 128
THETA = 10000
LOG2E = 1.4426950408889634
BLK = 256
HALF = BLK // 2
COLS = 512
ONES = 16
MESH = pl.DeviceIdType.MESH
BF, F32 = jnp.bfloat16, jnp.float32


def _dot(a, b, ca, cb):
    return lax.dot_general(a, b, (((ca,), (cb,)), ((), ())), preferred_element_type=F32)


def tables(rows):
    half = HEAD // 2
    angle = np.arange(rows)[:, None] * THETA ** (-np.arange(half) / half)
    cos, sin = np.cos(angle), np.sin(angle)
    return np.concatenate([cos, cos], 1).astype(np.float32), np.concatenate([-sin, sin], 1).astype(np.float32)


def kernel(nb, heads, x_h, gain_h, cos_h, sin_h, wq_h, wk_h, wv_h, wo_h, y_ref,
           gain_s, x_s, cos_s, sin_s, wq_s, wk_s, wv_s, wo_s, xn_s, q_s, k_s, v_s, s_s, top_s, mix_s, own_s,
           precv, csend, crecv,
           g_sem, x_sem, c_sem, s_sem, w_sem, ps_sem, pr_sem, cs_sem, cr_sem, fs_sem, fr_sem, r_sem):
    me = lax.axis_index("tp")
    core = lax.rem(me, 2)
    partner = me + 1 - 2 * core
    across = lax.rem(me + 2, 4)
    d = x_s.shape[2]
    nc = d // COLS
    width = heads * HEAD
    e = HEAD**-0.5 * LOG2E

    def rows(i):
        return pl.ds(pl.multiple_of(i * BLK, BLK), BLK)

    def mine(i):
        return pl.ds(pl.multiple_of(i * BLK + core * HALF, HALF), HALF)

    def cols(c):
        return pl.ds(c * COLS, COLS)

    class load:
        def __init__(self, i):
            at, here = lax.rem(i, 2), rows(jnp.minimum(i, nb - 1))
            self.copies = [pltpu.make_async_copy(a.at[here], b.at[at], sem.at[at])
                           for a, b, sem in ((x_h, x_s, x_sem), (cos_h, cos_s, c_sem), (sin_h, sin_s, s_sem))]

        def start(self):
            for c in self.copies:
                c.start()

        def wait(self):
            for c in self.copies:
                c.wait()

    def pieces(n, a, b):
        deep = a.shape[0] // 4
        return [pltpu.make_async_copy(a.at[pl.ds(m * deep, deep)], b.at[pl.ds(m * deep, deep)], w_sem.at[n]) for m in range(4)]

    def whole(n):
        pltpu.make_async_copy(given[n], kept[n], w_sem.at[n]).wait()

    given, kept = (wq_h, wk_h, wv_h, wo_h), (wq_s, wk_s, wv_s, wo_s)
    weights = [pieces(n, given[n], kept[n]) for n in range(4)]

    def fetch(n):
        for c in weights[n]:
            c.start()

    gain = pltpu.make_async_copy(gain_h, gain_s, g_sem)
    load(0).start()
    gain.start()
    fetch(0)

    barrier = pltpu.get_barrier_semaphore()
    for other in (partner, across):
        pl.semaphore_signal(barrier, inc=1, device_id={"tp": other}, device_id_type=MESH)

    v_s[:, :, HEAD:, :] = jnp.ones((nb, heads, ONES, BLK), BF)

    def to_partner(i, c):
        return pltpu.make_async_remote_copy(y_ref.at[mine(i), cols(c)], precv.at[i, :, cols(c)], ps_sem.at[lax.rem(i, 2), c], pr_sem.at[lax.rem(i, 2), c],
                                            device_id={"tp": partner}, device_id_type=MESH)

    def to_across(i, c):
        return pltpu.make_async_remote_copy(csend.at[i, c], crecv.at[i, c], cs_sem, cr_sem.at[i, c],
                                            device_id={"tp": across}, device_id_type=MESH)

    def final(i, c):
        return pltpu.make_async_remote_copy(y_ref.at[mine(i), cols(c)], y_ref.at[mine(i), cols(c)], fs_sem, fr_sem,
                                            device_id={"tp": partner}, device_id_type=MESH)

    def residual(i):
        return pltpu.make_async_copy(x_h.at[mine(i)], precv.at[i], r_sem.at[i])

    def chip_sum(i):
        for c in range(nc):
            to_partner(i, c).wait()
            csend[i, c] = (own_s[lax.rem(i, 2), c] + precv[i, :, c * COLS : (c + 1) * COLS].astype(F32)).astype(BF)
            to_across(i, c).start()
        residual(i).start()

    def norm(i):
        at = lax.rem(i, 2)
        for r in range(0, BLK, 32):
            wide = x_s[at, r : r + 32, :].astype(F32)
            scale = lax.rsqrt(jnp.mean(wide * wide, -1, keepdims=True) + 1e-6)
            xn_s[at, r : r + 32, :] = (wide * scale * gain_s[...].astype(F32)[None, :]).astype(BF)

    def turned(t, cos, sin):
        t = t.astype(BF).astype(F32)
        return (t * cos + pltpu.roll(t, HEAD // 2, 1) * sin).astype(BF)

    def scores(j, h):
        return _dot(k_s[j, h], q_s[h], 1, 1)

    def diagonal(i, more):
        ok = lax.broadcasted_iota(jnp.int32, (BLK, BLK), 0) <= lax.rem(lax.broadcasted_iota(jnp.int32, (BLK, BLK), 1) + core * HALF, BLK)
        found = [scores(i, h) for h in range(heads)]
        if more:
            for h in range(heads):
                s_s[0, h] = scores(0, h)
        ps = []
        for h, s in enumerate(found):
            s = jnp.where(ok, s, -1e30)
            top = s.max(axis=0, keepdims=True)
            top_s[h : h + 1, :] = top
            ps.append(jnp.exp2((s - top) * e).astype(BF))
        return ps

    def attend(j, _):
        now, later = lax.rem(j, 2), lax.rem(j + 1, 2)
        ps, keeps = [], []
        for h in range(heads):
            s_s[later, h] = scores(j + 1, h)
            s = s_s[now, h]
            old = top_s[h : h + 1, :]
            top = jnp.maximum(old, s.max(axis=0, keepdims=True))
            top_s[h : h + 1, :] = top
            keeps.append(jnp.exp2((old - top) * e))
            ps.append(jnp.exp2((s - top) * e).astype(BF))
        for h in range(heads):
            mix_s[h] = mix_s[h] * keeps[h] + _dot(v_s[j, h], ps[h], 1, 0)

    def block(i, start):
        now = lax.rem(i, 2)
        if not start:
            load(i + 1).start()
        cos, sin = cos_s[now], sin_s[now]
        xn = xn_s[now]
        for at in range(0, width, 256):
            if start:
                if at == 0:
                    whole(0)
                    fetch(2)
            t = _dot(xn, wq_s[:, at : at + 256], 1, 0)
            for n in range(2):
                turn = turned(t[:, n * HEAD : (n + 1) * HEAD], cos, sin)
                for m in range(2):
                    q_s[at // HEAD + n, pl.ds(pl.multiple_of(lax.rem(m + core, 2) * HALF, HALF), HALF), :] = turn[m * HALF : (m + 1) * HALF]
        for at in range(0, width, 256):
            if start:
                if at == 0:
                    whole(1)
                    fetch(3)
            t = _dot(xn, wk_s[:, at : at + 256], 1, 0)
            for n in range(2):
                k_s[i, at // HEAD + n] = turned(t[:, n * HEAD : (n + 1) * HEAD], cos, sin)
        ps = diagonal(i, not start)
        for at in range(0, width, 256):
            if start and at == 0:
                whole(2)
            t = _dot(xn, wv_s[:, at : at + 256], 1, 0).astype(BF).T
            for n in range(2):
                v_s[i, at // HEAD + n, :HEAD, :] = t[n * HEAD : (n + 1) * HEAD, :]

        for h in range(heads):
            mix_s[h] = _dot(v_s[i, h], ps[h], 1, 0)
        if not start:
            @pl.when(i > 1)
            def _():
                chip_sum(i - 1)

            lax.fori_loop(0, i, attend, None)
        if start:
            load(i + 1).start()
            pl.semaphore_wait(barrier, 2)
        else:
            load(i + 1).wait()
        seen = jnp.concatenate([(mix_s[h, :HEAD, :] * (1 / mix_s[h, HEAD : HEAD + 1, :])).astype(BF).T for h in range(heads)], axis=1)
        for c in range(nc):
            if start and c == 0:
                whole(3)
            part = _dot(seen, wo_s[:, c * COLS : (c + 1) * COLS], 1, 0)
            own_s[now, c] = part[:HALF]
            y_ref[mine(i), c * COLS : (c + 1) * COLS] = part[HALF:].astype(BF)
            if start:
                to_partner(i, c).start()
        if start:
            chip_sum(i)
            load(i + 1).wait()
        norm(i + 1)
        if not start:
            for c in range(nc):
                to_partner(i, c).start()

    load(0).wait()
    gain.wait()
    fetch(1)
    norm(0)
    block(0, True)

    def later(i, _):
        block(i, False)

    lax.fori_loop(1, nb, later, None)
    chip_sum(nb - 1)

    def finish(i, _):
        residual(i).wait()
        for c in range(nc):
            to_across(i, c).wait_recv()
            y_ref[mine(i), c * COLS : (c + 1) * COLS] = (
                precv[i, :, c * COLS : (c + 1) * COLS].astype(F32) + (csend[i, c].astype(F32) + crecv[i, c].astype(F32))).astype(BF)
            final(i, c).start()

    lax.fori_loop(0, nb, finish, None)

    pltpu.make_async_remote_copy(csend, crecv, cs_sem, cr_sem.at[0, 0], device_id={"tp": across}, device_id_type=MESH).wait_send()
    part = pl.ds(0, nb * HALF)
    pltpu.make_async_remote_copy(y_ref.at[part], y_ref.at[part], fs_sem, fr_sem, device_id={"tp": partner}, device_id_type=MESH).wait()


def solution(mesh):
    def step(x, gain, wq, wk, wv, wo):
        rows, d = x.shape
        width = wq.shape[1]
        heads, nb, nc = width // HEAD, rows // BLK, d // COLS
        cos, sin = (jnp.asarray(t) for t in tables(rows))
        anywhere, vmem, dma = pl.BlockSpec(memory_space=pl.ANY), pl.BlockSpec(memory_space=pltpu.VMEM), pltpu.SemaphoreType.DMA
        return pl.pallas_call(
            functools.partial(kernel, nb, heads),
            name="layer",
            out_shape=pltpu.VMEM((rows, d), BF),
            in_specs=[anywhere] * 8,
            out_specs=vmem,
            scratch_shapes=[
                pltpu.VMEM((d,), BF),
                pltpu.VMEM((2, BLK, d), BF), pltpu.VMEM((2, BLK, HEAD), F32), pltpu.VMEM((2, BLK, HEAD), F32),
                pltpu.VMEM((d, width), BF), pltpu.VMEM((d, width), BF), pltpu.VMEM((d, width), BF), pltpu.VMEM((width, d), BF),
                pltpu.VMEM((2, BLK, d), BF), pltpu.VMEM((heads, BLK, HEAD), BF), pltpu.VMEM((nb, heads, BLK, HEAD), BF),
                pltpu.VMEM((nb, heads, HEAD + ONES, BLK), BF), pltpu.VMEM((2, heads, BLK, BLK), F32), pltpu.VMEM((8, BLK), F32),
                pltpu.VMEM((heads, HEAD + ONES, BLK), F32),
                pltpu.VMEM((2, nc, HALF, COLS), F32),
                pltpu.VMEM((nb, HALF, d), BF), *[pltpu.VMEM((nb, nc, HALF, COLS), BF)] * 2,
                dma, dma((2,)), dma((2,)), dma((2,)), dma((4,)), dma((2, nc)), dma((2, nc)), dma, dma((nb, nc)), dma, dma, dma((nb,)),
            ],
            compiler_params=pltpu.CompilerParams(collective_id=0, has_side_effects=True, vmem_limit_bytes=55 * 2**20),
        )(x, gain, cos, sin, wq, wk, wv, wo)

    tokens, columns = P("dp", None), P(None, "tp")
    return jax.shard_map(
        step,
        mesh=mesh,
        in_specs=(tokens, P(None), columns, columns, columns, P("tp", None)),
        out_specs=tokens,
        check_vma=False,
    )
```

```python
import functools

import jax
import jax.numpy as jnp
import numpy as np
from jax import lax
from jax.experimental import pallas as pl
from jax.experimental.pallas import tpu as pltpu
from jax.sharding import PartitionSpec as P

HEAD = 128
THETA = 10000
LOG2E = 1.4426950408889634
BLK = 256
HALF = BLK // 2
COLS = 512
ONES = 16
MESH = pl.DeviceIdType.MESH
BF, F32 = jnp.bfloat16, jnp.float32


def _dot(a, b, ca, cb):
    return lax.dot_general(a, b, (((ca,), (cb,)), ((), ())), preferred_element_type=F32)


def tables(rows):
    half = HEAD // 2
    angle = np.arange(rows)[:, None] * THETA ** (-np.arange(half) / half)
    cos, sin = np.cos(angle), np.sin(angle)
    return np.concatenate([cos, cos, -sin, sin], 1).astype(np.float32)


def kernel(nb, heads, x_h, gain_h, turn_h, wq_h, wk_h, wv_h, wo_h, y_ref,
           gain_s, x_s, turn_s, wq_s, wk_s, wv_s, wo_s, xn_s, q_s, k_s, v_s, s_s, top_s, mix_s, own_s,
           precv, csend, crecv,
           g_sem, x_sem, t_sem, w_sem, v_sem, ps_sem, pr_sem, cs_sem, cr_sem, fs_sem, fr_sem, r_sem):
    me = lax.axis_index("tp")
    core = lax.rem(me, 2)
    partner = me + 1 - 2 * core
    across = lax.rem(me + 2, 4)
    d = x_s.shape[2]
    nc = d // COLS
    width = heads * HEAD
    e = HEAD**-0.5 * LOG2E

    def rows(i):
        return pl.ds(pl.multiple_of(i * BLK, BLK), BLK)

    def mine(i):
        return pl.ds(pl.multiple_of(i * BLK + core * HALF, HALF), HALF)

    def cols(c):
        return pl.ds(c * COLS, COLS)

    class load:
        def __init__(self, i):
            at, here = lax.rem(i, 2), jnp.minimum(i, nb - 1)
            piece = BLK // 8
            self.parts = [pltpu.make_async_copy(x_h.at[pl.ds(pl.multiple_of(here * BLK + m * piece, piece), piece)], x_s.at[at, pl.ds(m * piece, piece)],
                                                x_sem.at[at]) for m in range(8)]
            self.whole = pltpu.make_async_copy(x_h.at[rows(here)], x_s.at[at], x_sem.at[at])
            self.turn = pltpu.make_async_copy(turn_h.at[rows(here)], turn_s.at[at], t_sem.at[at])

        def start(self):
            for c in self.parts:
                c.start()

        def wait(self):
            self.whole.wait()

    def pieces(n, a, b):
        deep = a.shape[0] // 4
        return [pltpu.make_async_copy(a.at[pl.ds(m * deep, deep)], b.at[pl.ds(m * deep, deep)], v_sem.at[m] if n == 2 else w_sem.at[n]) for m in range(4)]

    def whole(n):
        pltpu.make_async_copy(given[n], held[n], w_sem.at[n]).wait()

    given, held = (wq_h, wk_h, wv_h, wo_h), (wq_s, wk_s, wv_s, wo_s)
    weights = [pieces(n, given[n], held[n]) for n in range(4)]

    def fetch(n):
        for c in weights[n]:
            c.start()

    gain = pltpu.make_async_copy(gain_h, gain_s, g_sem)
    load(0).start()
    gain.start()
    load(0).turn.start()
    fetch(0)

    barrier = pltpu.get_barrier_semaphore()
    for other in (partner, across):
        pl.semaphore_signal(barrier, inc=1, device_id={"tp": other}, device_id_type=MESH)

    v_s[:, :, HEAD:, :] = jnp.ones((nb, heads, ONES, BLK), BF)

    def places(i):
        if isinstance(i, int) and i == 0:
            return [(part * HALF + core * (HALF // 2), part * (HALF // 2), HALF // 2) for part in range(2)]
        return [(i * BLK + core * HALF, 0, HALF)]

    def ours(i, p):
        row, _, size = places(i)[p]
        return pl.ds(pl.multiple_of(row, size), size)

    def kept(i, p):
        _, at, size = places(i)[p]
        return pl.ds(at, size)

    def to_partner(i, c, p=0):
        slot = 2 * p if isinstance(i, int) and i == 0 else lax.rem(i, 2)
        return pltpu.make_async_remote_copy(y_ref.at[ours(i, p), cols(c)], precv.at[i, kept(i, p), cols(c)], ps_sem, pr_sem.at[slot, c],
                                            device_id={"tp": partner}, device_id_type=MESH)

    def to_across(i, c, p=0):
        return pltpu.make_async_remote_copy(csend.at[i, c, kept(i, p)], crecv.at[i, c, kept(i, p)], cs_sem, cr_sem.at[i + c * lax.div(i, nb - 1)],
                                            device_id={"tp": across}, device_id_type=MESH)

    def final(i, c, p=0):
        return pltpu.make_async_remote_copy(y_ref.at[ours(i, p), cols(c)], y_ref.at[ours(i, p), cols(c)], fs_sem, fr_sem,
                                            device_id={"tp": partner}, device_id_type=MESH)

    def residual(i, p=0):
        return pltpu.make_async_copy(x_h.at[ours(i, p)], precv.at[i, kept(i, p)], r_sem)

    def chip_sum(i, p=0):
        at = kept(i, p)
        for c in range(nc):
            to_partner(i, c, p).wait_recv()
            csend[i, c, at] = (own_s[lax.rem(i, 2), c, at] + precv[i, at, c * COLS : (c + 1) * COLS].astype(F32)).astype(BF)
            to_across(i, c, p).start()
        residual(i, p).start()

    def norm(i):
        at = lax.rem(i, 2)
        for r in range(0, BLK, 32):
            wide = x_s[at, r : r + 32, :].astype(F32)
            scale = lax.rsqrt(jnp.mean(wide * wide, -1, keepdims=True) + 1e-6)
            xn_s[at, r : r + 32, :] = (wide * scale * gain_s[...].astype(F32)[None, :]).astype(BF)

    def turned(t, cos, sin):
        t = t.astype(BF).astype(F32)
        return (t * cos + pltpu.roll(t, HEAD // 2, 1) * sin).astype(BF)

    def scores(j, h):
        return _dot(k_s[j, h], q_s[h], 1, 1)

    def diagonal(i, some, more):
        ok = lax.broadcasted_iota(jnp.int32, (BLK, BLK), 0) <= lax.rem(lax.broadcasted_iota(jnp.int32, (BLK, BLK), 1) + core * HALF, BLK)
        found = [scores(i, h) for h in some]
        if more:
            for h in some:
                s_s[0, h] = scores(0, h)
        ps = []
        for h, s in zip(some, found):
            s = jnp.where(ok, s, -1e30)
            top = s.max(axis=0, keepdims=True)
            top_s[h : h + 1, :] = top
            ps.append(jnp.exp2((s - top) * e).astype(BF))
        return ps

    def attend(j, _):
        now, later = lax.rem(j, 2), lax.rem(j + 1, 2)
        ps, keeps = [], []
        for h in range(heads):
            s_s[later, h] = scores(j + 1, h)
            s = s_s[now, h]
            old = top_s[h : h + 1, :]
            top = jnp.maximum(old, s.max(axis=0, keepdims=True))
            top_s[h : h + 1, :] = top
            keeps.append(jnp.exp2((old - top) * e))
            ps.append(jnp.exp2((s - top) * e).astype(BF))
        for h in range(heads):
            mix_s[h] = mix_s[h] * keeps[h] + _dot(v_s[j, h], ps[h], 1, 0)

    def first(p):
        keys = (p + 1) * HALF
        query = lax.rem(lax.broadcasted_iota(jnp.int32, (keys, HALF), 1) + core * (HALF // 2), HALF) + p * HALF
        ok = lax.broadcasted_iota(jnp.int32, (keys, HALF), 0) <= query
        ps = []
        for h in range(heads):
            s = jnp.where(ok, _dot(k_s[0, h, :keys, :], q_s[h, p * HALF : (p + 1) * HALF, :], 1, 1), -1e30)
            ps.append(jnp.exp2((s - s.max(axis=0, keepdims=True)) * e).astype(BF))
        return ps

    def start_up(ps):
        for p in range(2):
            mixed = [_dot(v_s[0, h, :, : (p + 1) * HALF], ps[h], 1, 0) for h in range(heads)]
            seen = jnp.concatenate([(m[:HEAD] * (1 / m[HEAD : HEAD + 1])).astype(BF).T for m in mixed], axis=1)
            if p == 0:
                load(1).start()
                load(1).turn.start()
                pl.semaphore_wait(barrier, 2)
                whole(3)
            for c in range(nc):
                part = _dot(seen, wo_s[:, c * COLS : (c + 1) * COLS], 1, 0)
                own_s[0, c, kept(0, p), :] = part[: HALF // 2]
                y_ref[ours(0, p), c * COLS : (c + 1) * COLS] = part[HALF // 2 :].astype(BF)
                to_partner(0, c, p).start()
            if p == 0:
                chip_sum(0, 0)
                ps = first(1)
        load(1).wait()
        load(1).turn.wait()
        norm(1)
        chip_sum(0, 1)

    def block(i, start):
        now = lax.rem(i, 2)
        if start:
            load(0).turn.wait()
        else:
            load(i + 1).start()
            load(i + 1).turn.start()
        cos, sin = turn_s[now, :, :HEAD], turn_s[now, :, HEAD:]
        xn = xn_s[now]
        for at in range(0, width, 256):
            if start:
                if at == 0:
                    whole(0)
                    fetch(2)
            t = _dot(xn, wq_s[:, at : at + 256], 1, 0)
            for n in range(2):
                turn = turned(t[:, n * HEAD : (n + 1) * HEAD], cos, sin)
                size = HALF // 2 if start else HALF
                for m in range(BLK // size):
                    to = m // 2 * HALF + lax.rem(m + core, 2) * size
                    q_s[at // HEAD + n, pl.ds(pl.multiple_of(to, size), size), :] = turn[m * size : (m + 1) * size]
        for at in range(0, width, 256):
            if start:
                if at == 0:
                    whole(1)
                    fetch(3)
            t = _dot(xn, wk_s[:, at : at + 256], 1, 0)
            for n in range(2):
                k_s[i, at // HEAD + n] = turned(t[:, n * HEAD : (n + 1) * HEAD], cos, sin)
        if start:
            for m in range(4):
                weights[2][m].wait()
            ps = first(0)
        else:
            @pl.when(i > 2)
            def _():
                chip_sum(i - 1)

            ps = diagonal(i, range(heads), True)
        for at in range(0, width, 256):
            t = _dot(xn, wv_s[:, at : at + 256], 1, 0).astype(BF).T
            for n in range(2):
                v_s[i, at // HEAD + n, :HEAD, :] = t[n * HEAD : (n + 1) * HEAD, :]
        if start:
            start_up(ps)
            return
        for h in range(heads):
            mix_s[h] = _dot(v_s[i, h], ps[h], 1, 0)
        lax.fori_loop(0, i, attend, None)
        load(i + 1).wait()
        load(i + 1).turn.wait()
        seen = jnp.concatenate([(mix_s[h, :HEAD, :] * (1 / mix_s[h, HEAD : HEAD + 1, :])).astype(BF).T for h in range(heads)], axis=1)
        for c in range(nc):
            part = _dot(seen, wo_s[:, c * COLS : (c + 1) * COLS], 1, 0)
            own_s[now, c] = part[:HALF]
            y_ref[mine(i), c * COLS : (c + 1) * COLS] = part[HALF:].astype(BF)
            to_partner(i, c).start()
        norm(i + 1)

        @pl.when(i == 1)
        def _():
            chip_sum(i)

    load(0).wait()
    gain.wait()
    fetch(1)
    norm(0)
    block(0, True)

    def later(i, _):
        block(i, False)

    lax.fori_loop(1, nb, later, None)
    chip_sum(nb - 1)

    part = pl.ds(0, nb * HALF)
    sent = pltpu.make_async_remote_copy(y_ref.at[part], y_ref.at[part], ps_sem, fr_sem, device_id={"tp": partner}, device_id_type=MESH)
    sent.wait_send()
    pltpu.make_async_copy(x_h.at[part], x_h.at[part], r_sem).wait()

    def finish(i, c, p=0):
        at = kept(i, p)
        y_ref[ours(i, p), c * COLS : (c + 1) * COLS] = (
            precv[i, at, c * COLS : (c + 1) * COLS].astype(F32) + (csend[i, c, at].astype(F32) + crecv[i, c, at].astype(F32))).astype(BF)
        final(i, c, p).start()

    def arrived(i):
        pltpu.make_async_remote_copy(csend.at[i], crecv.at[i], cs_sem, cr_sem.at[i], device_id={"tp": across}, device_id_type=MESH).wait_recv()

    arrived(0)
    for c in range(nc):
        for p in range(2):
            finish(0, c, p)

    def early(i, _):
        arrived(i)
        for c in range(nc):
            finish(i, c)

    lax.fori_loop(1, nb - 1, early, None)
    for c in range(nc):
        to_across(nb - 1, c).wait_recv()
        finish(nb - 1, c)

    pltpu.make_async_remote_copy(csend, crecv, cs_sem, cr_sem.at[0], device_id={"tp": across}, device_id_type=MESH).wait_send()
    pltpu.make_async_remote_copy(y_ref.at[part], y_ref.at[part], fs_sem, fr_sem, device_id={"tp": partner}, device_id_type=MESH).wait()


def solution(mesh):
    def step(x, gain, wq, wk, wv, wo):
        rows, d = x.shape
        width = wq.shape[1]
        heads, nb, nc = width // HEAD, rows // BLK, d // COLS
        turn = jnp.asarray(tables(rows))
        anywhere, vmem, dma = pl.BlockSpec(memory_space=pl.ANY), pl.BlockSpec(memory_space=pltpu.VMEM), pltpu.SemaphoreType.DMA
        return pl.pallas_call(
            functools.partial(kernel, nb, heads),
            name="layer",
            out_shape=pltpu.VMEM((rows, d), BF),
            in_specs=[anywhere] * 7,
            out_specs=vmem,
            scratch_shapes=[
                pltpu.VMEM((d,), BF),
                pltpu.VMEM((2, BLK, d), BF), pltpu.VMEM((2, BLK, 2 * HEAD), F32),
                pltpu.VMEM((d, width), BF), pltpu.VMEM((d, width), BF), pltpu.VMEM((d, width), BF), pltpu.VMEM((width, d), BF),
                pltpu.VMEM((2, BLK, d), BF), pltpu.VMEM((heads, BLK, HEAD), BF), pltpu.VMEM((nb, heads, BLK, HEAD), BF),
                pltpu.VMEM((nb, heads, HEAD + ONES, BLK), BF), pltpu.VMEM((2, heads, BLK, BLK), F32), pltpu.VMEM((8, BLK), F32),
                pltpu.VMEM((heads, HEAD + ONES, BLK), F32),
                pltpu.VMEM((2, nc, HALF, COLS), F32),
                pltpu.VMEM((nb, HALF, d), BF), *[pltpu.VMEM((nb, nc, HALF, COLS), BF)] * 2,
                dma, dma((2,)), dma((2,)), dma((4,)), dma((4,)), dma, dma((3, nc)), dma, dma((nb + nc - 1,)), dma, dma, dma,
            ],
            compiler_params=pltpu.CompilerParams(collective_id=0, has_side_effects=True, vmem_limit_bytes=55 * 2**20),
        )(x, gain, turn, wq, wk, wv, wo)

    tokens, columns = P("dp", None), P(None, "tp")
    return jax.shard_map(
        step,
        mesh=mesh,
        in_specs=(tokens, P(None), columns, columns, columns, P("tp", None)),
        out_specs=tokens,
        check_vma=False,
    )
```

```python
import functools

import jax
import jax.numpy as jnp
import numpy as np
from jax import lax
from jax.experimental import pallas as pl
from jax.experimental.pallas import tpu as pltpu
from jax.sharding import PartitionSpec as P

HEAD = 128
THETA = 10000
LOG2E = 1.4426950408889634
BLK = 256
HALF = BLK // 2
COLS = 512
ONES = 16
MESH = pl.DeviceIdType.MESH
BF, F32 = jnp.bfloat16, jnp.float32


def _dot(a, b, ca, cb):
    return lax.dot_general(a, b, (((ca,), (cb,)), ((), ())), preferred_element_type=F32)


def tables(rows):
    half = HEAD // 2
    angle = np.arange(rows)[:, None] * THETA ** (-np.arange(half) / half)
    cos, sin = np.cos(angle), np.sin(angle)
    return np.concatenate([cos, cos, -sin, sin], 1).astype(np.float32)


def kernel(nb, heads, x_h, gain_h, turn_h, wq_h, wk_h, wv_h, wo_h, y_ref,
           gain_s, x_s, turn_s, wq_s, wk_s, wv_s, wo_s, xn_s, q_s, k_s, v_s, s_s, top_s, mix_s, own_s,
           precv, csend, crecv,
           g_sem, x_sem, t_sem, w_sem, v_sem, ps_sem, pr_sem, cs_sem, cr_sem, fs_sem, fr_sem, r_sem):
    me = lax.axis_index("tp")
    core = lax.rem(me, 2)
    partner = me + 1 - 2 * core
    across = lax.rem(me + 2, 4)
    d = x_s.shape[2]
    nc = d // COLS
    width = heads * HEAD
    e = HEAD**-0.5 * LOG2E

    def rows(i):
        return pl.ds(pl.multiple_of(i * BLK, BLK), BLK)

    def mine(i):
        return pl.ds(pl.multiple_of(i * BLK + core * HALF, HALF), HALF)

    def cols(c):
        return pl.ds(c * COLS, COLS)

    class load:
        def __init__(self, i):
            at, here = lax.rem(i, 2), jnp.minimum(i, nb - 1)
            piece = BLK // 8
            self.parts = [pltpu.make_async_copy(x_h.at[pl.ds(pl.multiple_of(here * BLK + m * piece, piece), piece)], x_s.at[at, pl.ds(m * piece, piece)],
                                                x_sem.at[at]) for m in range(8)]
            self.whole = pltpu.make_async_copy(x_h.at[rows(here)], x_s.at[at], x_sem.at[at])
            self.turn = pltpu.make_async_copy(turn_h.at[rows(here)], turn_s.at[at], t_sem.at[at])

        def start(self):
            for c in self.parts:
                c.start()

        def wait(self):
            self.whole.wait()

    def pieces(n, a, b):
        deep = a.shape[0] // 4
        return [pltpu.make_async_copy(a.at[pl.ds(m * deep, deep)], b.at[pl.ds(m * deep, deep)], v_sem.at[m] if n == 2 else w_sem.at[n]) for m in range(4)]

    def whole(n):
        pltpu.make_async_copy(given[n], held[n], w_sem.at[n]).wait()

    given, held = (wq_h, wk_h, wv_h, wo_h), (wq_s, wk_s, wv_s, wo_s)
    weights = [pieces(n, given[n], held[n]) for n in range(4)]

    def fetch(n):
        for c in weights[n]:
            c.start()

    gain = pltpu.make_async_copy(gain_h, gain_s, g_sem)
    load(0).start()
    gain.start()
    load(0).turn.start()
    fetch(0)

    barrier = pltpu.get_barrier_semaphore()
    for other in (partner, across):
        pl.semaphore_signal(barrier, inc=1, device_id={"tp": other}, device_id_type=MESH)

    v_s[:, :, HEAD:, :] = jnp.ones((nb, heads, ONES, BLK), BF)

    def places(i):
        if isinstance(i, int) and i == 0:
            return [(part * HALF + core * (HALF // 2), part * (HALF // 2), HALF // 2) for part in range(2)]
        return [(i * BLK + core * HALF, 0, HALF)]

    def ours(i, p):
        row, _, size = places(i)[p]
        return pl.ds(pl.multiple_of(row, size), size)

    def kept(i, p):
        _, at, size = places(i)[p]
        return pl.ds(at, size)

    def to_partner(i, c, p=0):
        slot = 2 * p if isinstance(i, int) and i == 0 else lax.rem(i, 2)
        return pltpu.make_async_remote_copy(y_ref.at[ours(i, p), cols(c)], precv.at[i, kept(i, p), cols(c)], ps_sem, pr_sem.at[slot, c],
                                            device_id={"tp": partner}, device_id_type=MESH)

    def to_across(i, c, p=0):
        return pltpu.make_async_remote_copy(csend.at[i, c, kept(i, p)], crecv.at[i, c, kept(i, p)], cs_sem, cr_sem.at[i + c * lax.div(i, nb - 1)],
                                            device_id={"tp": across}, device_id_type=MESH)

    def final(i, c, p=0):
        return pltpu.make_async_remote_copy(y_ref.at[ours(i, p), cols(c)], y_ref.at[ours(i, p), cols(c)], fs_sem, fr_sem,
                                            device_id={"tp": partner}, device_id_type=MESH)

    def residual(i, p=0):
        return pltpu.make_async_copy(x_h.at[ours(i, p)], precv.at[i, kept(i, p)], r_sem)

    def chip_sum(i, p=0):
        at = kept(i, p)
        for c in range(nc):
            to_partner(i, c, p).wait_recv()
            csend[i, c, at] = (own_s[lax.rem(i, 2), c, at] + precv[i, at, c * COLS : (c + 1) * COLS].astype(F32)).astype(BF)
            to_across(i, c, p).start()
        residual(i, p).start()

    def norm(i):
        at = lax.rem(i, 2)
        for r in range(0, BLK, 32):
            wide = x_s[at, r : r + 32, :].astype(F32)
            scale = lax.rsqrt(jnp.mean(wide * wide, -1, keepdims=True) + 1e-6)
            xn_s[at, r : r + 32, :] = (wide * scale * gain_s[...].astype(F32)[None, :]).astype(BF)

    def turned(t, cos, sin):
        t = t.astype(BF).astype(F32)
        return (t * cos + pltpu.roll(t, HEAD // 2, 1) * sin).astype(BF)

    def scores(j, h):
        return _dot(k_s[j, h], q_s[h], 1, 1)

    def diagonal(i, some, more):
        ok = lax.broadcasted_iota(jnp.int32, (BLK, BLK), 0) <= lax.rem(lax.broadcasted_iota(jnp.int32, (BLK, BLK), 1) + core * HALF, BLK)
        found = [scores(i, h) for h in some]
        if more:
            for h in some:
                s_s[0, h] = scores(0, h)
        ps = []
        for h, s in zip(some, found):
            s = jnp.where(ok, s, -1e30)
            top = s.max(axis=0, keepdims=True)
            top_s[h : h + 1, :] = top
            ps.append(jnp.exp2((s - top) * e).astype(BF))
        return ps

    def attend(j, _):
        now, later = lax.rem(j, 2), lax.rem(j + 1, 2)
        ps, keeps = [], []
        for h in range(heads):
            s_s[later, h] = scores(j + 1, h)
            s = s_s[now, h]
            old = top_s[h : h + 1, :]
            top = jnp.maximum(old, s.max(axis=0, keepdims=True))
            top_s[h : h + 1, :] = top
            keeps.append(jnp.exp2((old - top) * e))
            ps.append(jnp.exp2((s - top) * e).astype(BF))
        for h in range(heads):
            mix_s[h] = mix_s[h] * keeps[h] + _dot(v_s[j, h], ps[h], 1, 0)

    def keys(i, some):
        now = lax.rem(i, 2)
        cos, sin = turn_s[now, some, :HEAD], turn_s[now, some, HEAD:]
        for at in range(0, width, 256):
            t = _dot(xn_s[now, some, :], wk_s[:, at : at + 256], 1, 0)
            for n in range(2):
                k_s[i, at // HEAD + n, some, :] = turned(t[:, n * HEAD : (n + 1) * HEAD], cos, sin)

    def values(i, some):
        for at in range(0, width, 256):
            t = _dot(xn_s[lax.rem(i, 2), some, :], wv_s[:, at : at + 256], 1, 0).astype(BF).T
            for n in range(2):
                v_s[i, at // HEAD + n, :HEAD, some] = t[n * HEAD : (n + 1) * HEAD, :]

    def first(p):
        keys = (p + 1) * HALF
        query = lax.rem(lax.broadcasted_iota(jnp.int32, (keys, HALF), 1) + core * (HALF // 2), HALF) + p * HALF
        ok = lax.broadcasted_iota(jnp.int32, (keys, HALF), 0) <= query
        ps = []
        for h in range(heads):
            s = jnp.where(ok, _dot(k_s[0, h, :keys, :], q_s[h, p * HALF : (p + 1) * HALF, :], 1, 1), -1e30)
            ps.append(jnp.exp2((s - s.max(axis=0, keepdims=True)) * e).astype(BF))
        return ps

    def start_up(ps):
        for p in range(2):
            mixed = [_dot(v_s[0, h, :, : (p + 1) * HALF], ps[h], 1, 0) for h in range(heads)]
            seen = jnp.concatenate([(m[:HEAD] * (1 / m[HEAD : HEAD + 1])).astype(BF).T for m in mixed], axis=1)
            if p == 0:
                load(1).start()
                load(1).turn.start()
                pl.semaphore_wait(barrier, 2)
                whole(3)
            for c in range(nc):
                part = _dot(seen, wo_s[:, c * COLS : (c + 1) * COLS], 1, 0)
                own_s[0, c, kept(0, p), :] = part[: HALF // 2]
                y_ref[ours(0, p), c * COLS : (c + 1) * COLS] = part[HALF // 2 :].astype(BF)
                to_partner(0, c, p).start()
            if p == 0:
                keys(0, slice(HALF, BLK))
                chip_sum(0, 0)
                ps = first(1)
                values(0, slice(HALF, BLK))
        load(1).wait()
        load(1).turn.wait()
        norm(1)
        chip_sum(0, 1)

    def block(i, start):
        now = lax.rem(i, 2)
        if start:
            load(0).turn.wait()
        else:
            load(i + 1).start()
            load(i + 1).turn.start()
        cos, sin = turn_s[now, :, :HEAD], turn_s[now, :, HEAD:]
        xn = xn_s[now]
        for at in range(0, width, 256):
            if start:
                if at == 0:
                    whole(0)
                    fetch(2)
            t = _dot(xn, wq_s[:, at : at + 256], 1, 0)
            for n in range(2):
                turn = turned(t[:, n * HEAD : (n + 1) * HEAD], cos, sin)
                size = HALF // 2 if start else HALF
                for m in range(BLK // size):
                    to = m // 2 * HALF + lax.rem(m + core, 2) * size
                    q_s[at // HEAD + n, pl.ds(pl.multiple_of(to, size), size), :] = turn[m * size : (m + 1) * size]
        if start:
            whole(1)
            fetch(3)
        keys(i, slice(0, HALF) if start else slice(0, BLK))
        if start:
            for m in range(4):
                weights[2][m].wait()
            ps = first(0)
        else:
            @pl.when(i > 2)
            def _():
                chip_sum(i - 1)

            ps = diagonal(i, range(heads), True)
        values(i, slice(0, HALF) if start else slice(0, BLK))
        if start:
            start_up(ps)
            return
        for h in range(heads):
            mix_s[h] = _dot(v_s[i, h], ps[h], 1, 0)
        lax.fori_loop(0, i, attend, None)
        load(i + 1).wait()
        load(i + 1).turn.wait()
        seen = jnp.concatenate([(mix_s[h, :HEAD, :] * (1 / mix_s[h, HEAD : HEAD + 1, :])).astype(BF).T for h in range(heads)], axis=1)
        for c in range(nc):
            part = _dot(seen, wo_s[:, c * COLS : (c + 1) * COLS], 1, 0)
            own_s[now, c] = part[:HALF]
            y_ref[mine(i), c * COLS : (c + 1) * COLS] = part[HALF:].astype(BF)
            to_partner(i, c).start()
        norm(i + 1)

        @pl.when(i == 1)
        def _():
            chip_sum(i)

    load(0).wait()
    gain.wait()
    fetch(1)
    norm(0)
    block(0, True)

    def later(i, _):
        block(i, False)

    lax.fori_loop(1, nb, later, None)
    chip_sum(nb - 1)

    part = pl.ds(0, nb * HALF)
    sent = pltpu.make_async_remote_copy(y_ref.at[part], y_ref.at[part], ps_sem, fr_sem, device_id={"tp": partner}, device_id_type=MESH)
    sent.wait_send()
    pltpu.make_async_copy(x_h.at[part], x_h.at[part], r_sem).wait()

    def finish(i, c, p=0):
        at = kept(i, p)
        y_ref[ours(i, p), c * COLS : (c + 1) * COLS] = (
            precv[i, at, c * COLS : (c + 1) * COLS].astype(F32) + (csend[i, c, at].astype(F32) + crecv[i, c, at].astype(F32))).astype(BF)
        final(i, c, p).start()

    def arrived(i):
        pltpu.make_async_remote_copy(csend.at[i], crecv.at[i], cs_sem, cr_sem.at[i], device_id={"tp": across}, device_id_type=MESH).wait_recv()

    arrived(0)
    for c in range(nc):
        for p in range(2):
            finish(0, c, p)

    def early(i, _):
        arrived(i)
        for c in range(nc):
            finish(i, c)

    lax.fori_loop(1, nb - 1, early, None)
    for c in range(nc):
        to_across(nb - 1, c).wait_recv()
        finish(nb - 1, c)

    pltpu.make_async_remote_copy(csend, crecv, cs_sem, cr_sem.at[0], device_id={"tp": across}, device_id_type=MESH).wait_send()
    pltpu.make_async_remote_copy(y_ref.at[part], y_ref.at[part], fs_sem, fr_sem, device_id={"tp": partner}, device_id_type=MESH).wait()


def solution(mesh):
    def step(x, gain, wq, wk, wv, wo):
        rows, d = x.shape
        width = wq.shape[1]
        heads, nb, nc = width // HEAD, rows // BLK, d // COLS
        turn = jnp.asarray(tables(rows))
        anywhere, vmem, dma = pl.BlockSpec(memory_space=pl.ANY), pl.BlockSpec(memory_space=pltpu.VMEM), pltpu.SemaphoreType.DMA
        return pl.pallas_call(
            functools.partial(kernel, nb, heads),
            name="layer",
            out_shape=pltpu.VMEM((rows, d), BF),
            in_specs=[anywhere] * 7,
            out_specs=vmem,
            scratch_shapes=[
                pltpu.VMEM((d,), BF),
                pltpu.VMEM((2, BLK, d), BF), pltpu.VMEM((2, BLK, 2 * HEAD), F32),
                pltpu.VMEM((d, width), BF), pltpu.VMEM((d, width), BF), pltpu.VMEM((d, width), BF), pltpu.VMEM((width, d), BF),
                pltpu.VMEM((2, BLK, d), BF), pltpu.VMEM((heads, BLK, HEAD), BF), pltpu.VMEM((nb, heads, BLK, HEAD), BF),
                pltpu.VMEM((nb, heads, HEAD + ONES, BLK), BF), pltpu.VMEM((2, heads, BLK, BLK), F32), pltpu.VMEM((8, BLK), F32),
                pltpu.VMEM((heads, HEAD + ONES, BLK), F32),
                pltpu.VMEM((2, nc, HALF, COLS), F32),
                pltpu.VMEM((nb, HALF, d), BF), *[pltpu.VMEM((nb, nc, HALF, COLS), BF)] * 2,
                dma, dma((2,)), dma((2,)), dma((4,)), dma((4,)), dma, dma((3, nc)), dma, dma((nb + nc - 1,)), dma, dma, dma,
            ],
            compiler_params=pltpu.CompilerParams(collective_id=0, has_side_effects=True, vmem_limit_bytes=55 * 2**20),
        )(x, gain, turn, wq, wk, wv, wo)

    tokens, columns = P("dp", None), P(None, "tp")
    return jax.shard_map(
        step,
        mesh=mesh,
        in_specs=(tokens, P(None), columns, columns, columns, P("tp", None)),
        out_specs=tokens,
        check_vma=False,
    )
```

```python
import functools

import jax
import jax.numpy as jnp
import numpy as np
from jax import lax
from jax.experimental import pallas as pl
from jax.experimental.pallas import tpu as pltpu
from jax.sharding import PartitionSpec as P

HEAD = 128
THETA = 10000
LOG2E = 1.4426950408889634
BLK = 256
HALF = BLK // 2
COLS = 512
ONES = 16
MESH = pl.DeviceIdType.MESH
BF, F32 = jnp.bfloat16, jnp.float32


def _dot(a, b, ca, cb):
    return lax.dot_general(a, b, (((ca,), (cb,)), ((), ())), preferred_element_type=F32)


def tables(rows):
    half = HEAD // 2
    angle = np.arange(rows)[:, None] * THETA ** (-np.arange(half) / half)
    cos, sin = np.cos(angle), np.sin(angle)
    return np.concatenate([cos, cos, -sin, sin], 1).astype(np.float32)


def kernel(nb, heads, x_h, gain_h, turn_h, wq_h, wk_h, wv_h, wo_h, y_ref,
           gain_s, x_s, turn_s, wq_s, wk_s, wv_s, wo_s, xn_s, q_s, k_s, v_s, s_s, top_s, mix_s, own_s,
           precv, csend, crecv,
           g_sem, x_sem, t_sem, w_sem, v_sem, ps_sem, pr_sem, cs_sem, cr_sem, fs_sem, fr_sem, r_sem):
    me = lax.axis_index("tp")
    core = lax.rem(me, 2)
    partner = me + 1 - 2 * core
    across = lax.rem(me + 2, 4)
    d = x_s.shape[2]
    nc = d // COLS
    width = heads * HEAD
    e = HEAD**-0.5 * LOG2E

    def rows(i):
        return pl.ds(pl.multiple_of(i * BLK, BLK), BLK)

    def mine(i):
        return pl.ds(pl.multiple_of(i * BLK + core * HALF, HALF), HALF)

    def cols(c):
        return pl.ds(c * COLS, COLS)

    class load:
        def __init__(self, i):
            at, here = lax.rem(i, 2), jnp.minimum(i, nb - 1)
            piece = BLK // 8
            self.parts = [pltpu.make_async_copy(x_h.at[pl.ds(pl.multiple_of(here * BLK + m * piece, piece), piece)], x_s.at[at, pl.ds(m * piece, piece)],
                                                x_sem.at[at]) for m in range(8)]
            self.whole = pltpu.make_async_copy(x_h.at[rows(here)], x_s.at[at], x_sem.at[at])
            self.turn = pltpu.make_async_copy(turn_h.at[rows(here)], turn_s.at[at], t_sem.at[at])

        def start(self):
            for c in self.parts:
                c.start()

        def wait(self):
            self.whole.wait()

    def pieces(n, a, b):
        deep = a.shape[0] // 4
        return [pltpu.make_async_copy(a.at[pl.ds(m * deep, deep)], b.at[pl.ds(m * deep, deep)], v_sem.at[m] if n == 2 else w_sem.at[n]) for m in range(4)]

    def whole(n):
        pltpu.make_async_copy(given[n], held[n], w_sem.at[n]).wait()

    given, held = (wq_h, wk_h, wv_h, wo_h), (wq_s, wk_s, wv_s, wo_s)
    weights = [pieces(n, given[n], held[n]) for n in range(4)]

    def fetch(n):
        for c in weights[n]:
            c.start()

    gain = pltpu.make_async_copy(gain_h, gain_s, g_sem)
    load(0).start()
    gain.start()
    load(0).turn.start()
    fetch(0)

    barrier = pltpu.get_barrier_semaphore()
    for other in (partner, across):
        pl.semaphore_signal(barrier, inc=1, device_id={"tp": other}, device_id_type=MESH)

    v_s[:, :, HEAD:, :] = jnp.ones((nb, heads, ONES, BLK), BF)

    def places(i):
        if isinstance(i, int) and i == 0:
            return [(part * HALF + core * (HALF // 2), part * (HALF // 2), HALF // 2) for part in range(2)]
        return [(i * BLK + core * HALF, 0, HALF)]

    def ours(i, p):
        row, _, size = places(i)[p]
        return pl.ds(pl.multiple_of(row, size), size)

    def kept(i, p):
        _, at, size = places(i)[p]
        return pl.ds(at, size)

    def to_partner(i, c, p=0):
        slot = 2 * p if isinstance(i, int) and i == 0 else lax.rem(i, 2)
        return pltpu.make_async_remote_copy(y_ref.at[ours(i, p), cols(c)], precv.at[i, kept(i, p), cols(c)], ps_sem, pr_sem.at[slot, c],
                                            device_id={"tp": partner}, device_id_type=MESH)

    def to_across(i, c, p=0):
        return pltpu.make_async_remote_copy(csend.at[i, c, kept(i, p)], crecv.at[i, c, kept(i, p)], cs_sem, cr_sem.at[i + c * lax.div(i, nb - 1)],
                                            device_id={"tp": across}, device_id_type=MESH)

    def final(i, c, p=0):
        return pltpu.make_async_remote_copy(y_ref.at[ours(i, p), cols(c)], y_ref.at[ours(i, p), cols(c)], fs_sem, fr_sem,
                                            device_id={"tp": partner}, device_id_type=MESH)

    def residual(i, p=0):
        return pltpu.make_async_copy(x_h.at[ours(i, p)], precv.at[i, kept(i, p)], r_sem)

    def chip_sum(i, p=0):
        at = kept(i, p)
        for c in range(nc):
            to_partner(i, c, p).wait_recv()
            csend[i, c, at] = (own_s[lax.rem(i, 2), c, at] + precv[i, at, c * COLS : (c + 1) * COLS].astype(F32)).astype(BF)
            to_across(i, c, p).start()
        residual(i, p).start()

    def norm(i):
        at = lax.rem(i, 2)
        for r in range(0, BLK, 32):
            wide = x_s[at, r : r + 32, :].astype(F32)
            scale = lax.rsqrt(jnp.mean(wide * wide, -1, keepdims=True) + 1e-6)
            xn_s[at, r : r + 32, :] = (wide * scale * gain_s[...].astype(F32)[None, :]).astype(BF)

    def turned(t, cos, sin):
        t = t.astype(BF).astype(F32)
        return (t * cos + pltpu.roll(t, HEAD // 2, 1) * sin).astype(BF)

    def scores(j, h):
        return _dot(k_s[j, h], q_s[h], 1, 1)

    def diagonal(i, some, more):
        ok = lax.broadcasted_iota(jnp.int32, (BLK, BLK), 0) <= lax.rem(lax.broadcasted_iota(jnp.int32, (BLK, BLK), 1) + core * HALF, BLK)
        found = [scores(i, h) for h in some]
        if more:
            for h in some:
                s_s[0, h] = scores(0, h)
        ps = []
        for h, s in zip(some, found):
            s = jnp.where(ok, s, -1e30)
            top = s.max(axis=0, keepdims=True)
            top_s[h : h + 1, :] = top
            ps.append(jnp.exp2((s - top) * e).astype(BF))
        return ps

    def attend(j, _):
        now, later = lax.rem(j, 2), lax.rem(j + 1, 2)
        ps, keeps = [], []
        for h in range(heads):
            s_s[later, h] = scores(j + 1, h)
            s = s_s[now, h]
            old = top_s[h : h + 1, :]
            top = jnp.maximum(old, s.max(axis=0, keepdims=True))
            top_s[h : h + 1, :] = top
            keeps.append(jnp.exp2((old - top) * e))
            ps.append(jnp.exp2((s - top) * e).astype(BF))
        for h in range(heads):
            mix_s[h] = mix_s[h] * keeps[h] + _dot(v_s[j, h], ps[h], 1, 0)

    def keys(i, some):
        now = lax.rem(i, 2)
        cos, sin = turn_s[now, some, :HEAD], turn_s[now, some, HEAD:]
        for at in range(0, width, 256):
            t = _dot(xn_s[now, some, :], wk_s[:, at : at + 256], 1, 0)
            for n in range(2):
                k_s[i, at // HEAD + n, some, :] = turned(t[:, n * HEAD : (n + 1) * HEAD], cos, sin)

    def values(i, some):
        for at in range(0, width, 256):
            t = _dot(xn_s[lax.rem(i, 2), some, :], wv_s[:, at : at + 256], 1, 0).astype(BF).T
            for n in range(2):
                v_s[i, at // HEAD + n, :HEAD, some] = t[n * HEAD : (n + 1) * HEAD, :]

    def first(p):
        keys = (p + 1) * HALF
        query = lax.rem(lax.broadcasted_iota(jnp.int32, (keys, HALF), 1) + core * (HALF // 2), HALF) + p * HALF
        ok = lax.broadcasted_iota(jnp.int32, (keys, HALF), 0) <= query
        ps = []
        for h in range(heads):
            s = jnp.where(ok, _dot(k_s[0, h, :keys, :], q_s[h, p * HALF : (p + 1) * HALF, :], 1, 1), -1e30)
            ps.append(jnp.exp2((s - s.max(axis=0, keepdims=True)) * e).astype(BF))
        return ps

    def start_up(ps):
        for p in range(2):
            mixed = [_dot(v_s[0, h, :, : (p + 1) * HALF], ps[h], 1, 0) for h in range(heads)]
            seen = jnp.concatenate([(m[:HEAD] * (1 / m[HEAD : HEAD + 1])).astype(BF).T for m in mixed], axis=1)
            if p == 0:
                load(1).start()
                load(1).turn.start()
                pl.semaphore_wait(barrier, 2)
                whole(3)
            for c in range(nc):
                part = _dot(seen, wo_s[:, c * COLS : (c + 1) * COLS], 1, 0)
                own_s[0, c, kept(0, p), :] = part[: HALF // 2]
                y_ref[ours(0, p), c * COLS : (c + 1) * COLS] = part[HALF // 2 :].astype(BF)
                to_partner(0, c, p).start()
            if p == 0:
                values(0, slice(HALF, BLK))
                chip_sum(0, 0)
                keys(0, slice(HALF, BLK))
                ps = first(1)
        load(1).wait()
        load(1).turn.wait()
        norm(1)
        chip_sum(0, 1)

    def block(i, start):
        now = lax.rem(i, 2)
        if start:
            load(0).turn.wait()
        else:
            load(i + 1).start()
            load(i + 1).turn.start()
        cos, sin = turn_s[now, :, :HEAD], turn_s[now, :, HEAD:]
        xn = xn_s[now]
        for at in range(0, width, 256):
            if start:
                if at == 0:
                    whole(0)
                    fetch(2)
            t = _dot(xn, wq_s[:, at : at + 256], 1, 0)
            for n in range(2):
                turn = turned(t[:, n * HEAD : (n + 1) * HEAD], cos, sin)
                size = HALF // 2 if start else HALF
                for m in range(BLK // size):
                    to = m // 2 * HALF + lax.rem(m + core, 2) * size
                    q_s[at // HEAD + n, pl.ds(pl.multiple_of(to, size), size), :] = turn[m * size : (m + 1) * size]
        if start:
            whole(1)
            fetch(3)
        keys(i, slice(0, HALF) if start else slice(0, BLK))
        if start:
            for m in range(4):
                weights[2][m].wait()
            ps = first(0)
        else:
            @pl.when(i > 2)
            def _():
                chip_sum(i - 1)

            ps = diagonal(i, range(heads), True)
        values(i, slice(0, HALF) if start else slice(0, BLK))
        if start:
            start_up(ps)
            return
        for h in range(heads):
            mix_s[h] = _dot(v_s[i, h], ps[h], 1, 0)
        lax.fori_loop(0, i, attend, None)
        load(i + 1).wait()
        load(i + 1).turn.wait()
        seen = jnp.concatenate([(mix_s[h, :HEAD, :] * (1 / mix_s[h, HEAD : HEAD + 1, :])).astype(BF).T for h in range(heads)], axis=1)
        for c in range(nc):
            part = _dot(seen, wo_s[:, c * COLS : (c + 1) * COLS], 1, 0)
            own_s[now, c] = part[:HALF]
            y_ref[mine(i), c * COLS : (c + 1) * COLS] = part[HALF:].astype(BF)
            to_partner(i, c).start()
        norm(i + 1)

        @pl.when(i == 1)
        def _():
            chip_sum(i)

    load(0).wait()
    gain.wait()
    fetch(1)
    norm(0)
    block(0, True)

    def later(i, _):
        block(i, False)

    lax.fori_loop(1, nb, later, None)
    chip_sum(nb - 1)

    part = pl.ds(0, nb * HALF)
    sent = pltpu.make_async_remote_copy(y_ref.at[part], y_ref.at[part], ps_sem, fr_sem, device_id={"tp": partner}, device_id_type=MESH)
    sent.wait_send()
    pltpu.make_async_copy(x_h.at[part], x_h.at[part], r_sem).wait()

    def finish(i, c, p=0):
        at = kept(i, p)
        y_ref[ours(i, p), c * COLS : (c + 1) * COLS] = (
            precv[i, at, c * COLS : (c + 1) * COLS].astype(F32) + (csend[i, c, at].astype(F32) + crecv[i, c, at].astype(F32))).astype(BF)
        final(i, c, p).start()

    def arrived(i):
        pltpu.make_async_remote_copy(csend.at[i], crecv.at[i], cs_sem, cr_sem.at[i], device_id={"tp": across}, device_id_type=MESH).wait_recv()

    arrived(0)
    for c in range(nc):
        for p in range(2):
            finish(0, c, p)

    def early(i, _):
        arrived(i)
        for c in range(nc):
            finish(i, c)

    lax.fori_loop(1, nb - 1, early, None)
    for c in range(nc):
        to_across(nb - 1, c).wait_recv()
        finish(nb - 1, c)

    pltpu.make_async_remote_copy(csend, crecv, cs_sem, cr_sem.at[0], device_id={"tp": across}, device_id_type=MESH).wait_send()
    pltpu.make_async_remote_copy(y_ref.at[part], y_ref.at[part], fs_sem, fr_sem, device_id={"tp": partner}, device_id_type=MESH).wait()


def solution(mesh):
    def step(x, gain, wq, wk, wv, wo):
        rows, d = x.shape
        width = wq.shape[1]
        heads, nb, nc = width // HEAD, rows // BLK, d // COLS
        turn = jnp.asarray(tables(rows))
        anywhere, vmem, dma = pl.BlockSpec(memory_space=pl.ANY), pl.BlockSpec(memory_space=pltpu.VMEM), pltpu.SemaphoreType.DMA
        return pl.pallas_call(
            functools.partial(kernel, nb, heads),
            name="layer",
            out_shape=pltpu.VMEM((rows, d), BF),
            in_specs=[anywhere] * 7,
            out_specs=vmem,
            scratch_shapes=[
                pltpu.VMEM((d,), BF),
                pltpu.VMEM((2, BLK, d), BF), pltpu.VMEM((2, BLK, 2 * HEAD), F32),
                pltpu.VMEM((d, width), BF), pltpu.VMEM((d, width), BF), pltpu.VMEM((d, width), BF), pltpu.VMEM((width, d), BF),
                pltpu.VMEM((2, BLK, d), BF), pltpu.VMEM((heads, BLK, HEAD), BF), pltpu.VMEM((nb, heads, BLK, HEAD), BF),
                pltpu.VMEM((nb, heads, HEAD + ONES, BLK), BF), pltpu.VMEM((2, heads, BLK, BLK), F32), pltpu.VMEM((8, BLK), F32),
                pltpu.VMEM((heads, HEAD + ONES, BLK), F32),
                pltpu.VMEM((2, nc, HALF, COLS), F32),
                pltpu.VMEM((nb, HALF, d), BF), *[pltpu.VMEM((nb, nc, HALF, COLS), BF)] * 2,
                dma, dma((2,)), dma((2,)), dma((4,)), dma((4,)), dma, dma((3, nc)), dma, dma((nb + nc - 1,)), dma, dma, dma,
            ],
            compiler_params=pltpu.CompilerParams(collective_id=0, has_side_effects=True, vmem_limit_bytes=55 * 2**20),
        )(x, gain, turn, wq, wk, wv, wo)

    tokens, columns = P("dp", None), P(None, "tp")
    return jax.shard_map(
        step,
        mesh=mesh,
        in_specs=(tokens, P(None), columns, columns, columns, P("tp", None)),
        out_specs=tokens,
        check_vma=False,
    )
```
